768 devices in a mesh: blk: 128 (over y, z_hi, x), grp: 6 (over z_lo, core).
Axes of the slice: x: 4, y: 8, z: 12 (z_hi: 4, z_lo: 3; z = z_hi * 3 + z_lo), core: 2. Of those that a mesh axis runs over, the one named last changes fastest.
Arguments:
- text: bfloat16 [128, 1152, 1024], P('blk', 'grp'), may hold values from -64 to 64
- image: bfloat16 [128, 1152, 1024], P('blk', 'grp'), may hold values from -64 to 64
- pair_index: int32 [128, 1152], P('blk', 'grp'), may hold values from 0 to 1151, each once within a row
Outputs:
- grad_text: float32 [128, 1152, 1024], P('blk', 'grp')
- grad_image: float32 [128, 1152, 1024], P('blk', 'grp')
- loss: float32 [], replicated
The draws below stay inside these ranges and needn't reach their ends.
Inputs may be any that keep to these rules, and one draw needn't show every extreme that they name: Every sub-batch's row of pair_index names each of 0 to 1151 once.
All inputs are finite; a program needn't handle non-finite values.
Results may differ from the reference program's by a relative error of at most 0.0024.
Values may be sent and summed in bfloat16 or wider, within the bound.
A program may use at most 32 MiB of HBM per device.

```python
import jax
import jax.numpy as jnp

D = 1024
SUB = 1152
GROUPS = 128


def embed_pair(key):
    key = jax.random.fold_in(key, 7)
    keys = jax.random.split(key, 6)
    text_base = jax.random.normal(keys[0], (GROUPS, SUB, D), jnp.float32)
    image_base = jax.random.normal(keys[1], (GROUPS, SUB, D), jnp.float32)
    text_out = text_base
    image_out = image_base
    targets = (110.0, 150.0, 200.0, 260.0)
    for number in range(4):
        target = targets[number]
        first_row = number * (SUB // 4)
        base = image_base[:, first_row + 1]
        noise_a = jax.random.normal(jax.random.fold_in(keys[4], number), (GROUPS, D), jnp.float32)
        noise_b = jax.random.normal(jax.random.fold_in(keys[5], number), (GROUPS, D), jnp.float32)
        base_sq = jnp.sum(base * base, axis=-1, keepdims=True)
        perp_a = noise_a - jnp.sum(noise_a * base, axis=-1, keepdims=True) / base_sq * base
        perp_b = noise_b - jnp.sum(noise_b * base, axis=-1, keepdims=True) / base_sq * base
        stretch = jnp.sqrt(target / (0.125 * base_sq))
        aligned = stretch * base
        shrink = 1.0 - 2.0 / target
        image_out = image_out.at[:, first_row + 1].set(aligned)
        image_out = image_out.at[:, first_row + 2].set(shrink * aligned + perp_a)
        text_out = text_out.at[:, first_row].set(aligned)
        text_out = text_out.at[:, first_row + 1].set(shrink * aligned + perp_b)
    return (jnp.clip(text_out, -64.0, 64.0), jnp.clip(image_out, -64.0, 64.0))


def draw_text(key, part):
    return embed_pair(key)[0].astype(jnp.bfloat16)


def draw_image(key, part):
    return embed_pair(key)[1].astype(jnp.bfloat16)


def setup_inputs(seed: int = 0) -> dict:
    key_of = jax.random.split(jax.random.key(seed), 4)
    return {
        "text": draw_text(jax.random.fold_in(key_of[3], 71), 0),
        "image": draw_image(jax.random.fold_in(key_of[3], 71), 0),
        "pair_index": jax.vmap(lambda own: jax.random.permutation(own, SUB))(jax.random.split(key_of[2], GROUPS)).reshape((GROUPS, SUB)).astype(jnp.int32),
    }


score_scale = 0.125


def group_terms(text_rows, image_rows, pairs):
    scores = jnp.dot(text_rows, image_rows.T, preferred_element_type=jnp.float32) * score_scale
    row_top = jnp.max(scores, axis=1)
    row_lse = row_top + jnp.log(jnp.sum(jnp.exp(scores - row_top[:, None]), axis=1))
    col_top = jnp.max(scores, axis=0)
    col_lse = col_top + jnp.log(jnp.sum(jnp.exp(scores - col_top[None, :]), axis=0))
    hit = pairs[:, None] == jnp.arange(SUB, dtype=jnp.int32)[None, :]
    positive = jnp.sum(jnp.where(hit, scores, 0.0), axis=1)
    weight = (jnp.exp(scores - row_lse[:, None]) + jnp.exp(scores - col_lse[None, :]) - 2.0 * hit.astype(jnp.float32)).astype(jnp.bfloat16)
    grad_t = jnp.dot(weight, image_rows, preferred_element_type=jnp.float32) * (score_scale * 0.5)
    grad_i = jnp.dot(weight.T, text_rows, preferred_element_type=jnp.float32) * (score_scale * 0.5)
    partial_sum = jnp.sum(row_lse - 2.0 * positive) + jnp.sum(col_lse)
    return grad_t, grad_i, partial_sum


def reference(text, image, pair_index):
    grads_t = []
    grads_i = []
    total = jnp.zeros((), jnp.float32)
    for group in range(GROUPS):
        grad_t, grad_i, partial_sum = group_terms(text[group], image[group], pair_index[group])
        grads_t.append(grad_t)
        grads_i.append(grad_i)
        total = total + partial_sum
    loss = total / (2.0 * SUB * GROUPS)
    return jnp.stack(grads_t), jnp.stack(grads_i), loss
```

```python
import functools

import jax
import jax.numpy as jnp
from jax import lax
from jax.experimental import pallas as pl
from jax.experimental.pallas import tpu as pltpu
from jax.sharding import Mesh
from jax.sharding import PartitionSpec as P

GRP = ("grp_0", "grp_1")
BLK = ("blk_0", "blk_1", "blk_2")
MESH = pl.DeviceIdType.MESH
F32 = jnp.float32
BF16 = jnp.bfloat16

SCALE = 0.125
LANES = 128
R = 64
NC = 3
KS = 2
ZS = 3
ROWS = R * NC
BLOCK = R * KS
TOTAL = ROWS * KS * ZS
MIDW = NC * BLOCK
NT = TOTAL // LANES
REDUCE = ("blk_1", "blk_2", "blk_0")


def mid_base(n):
    return n * BLOCK


def end_base(z, n):
    return MIDW + n * 2 * BLOCK + (z // 2) * BLOCK


def row_ids(q):
    in_mid = q < MIDW
    e = q - MIDW
    n = jnp.where(in_mid, q >> 7, e >> 8)
    z = jnp.where(in_mid, 1, ((e >> 7) & 1) * 2)
    k = (q >> 6) & 1
    return (z * KS + k) * ROWS + n * R + (q & (R - 1))


def fold(x, op):
    parts = [x[8 * i : 8 * i + 8] for i in range(x.shape[0] // 8)]
    while len(parts) > 1:
        parts = [op(parts[i], parts[i + 1]) if i + 1 < len(parts) else parts[i] for i in range(0, len(parts), 2)]
    return parts[0]


def tree(parts, op):
    parts = list(parts)
    while len(parts) > 1:
        parts = [op(parts[i], parts[i + 1]) if i + 1 < len(parts) else parts[i] for i in range(0, len(parts), 2)]
    return parts[0]


def add(a, b):
    return a + b


def dot_nt(a, b):
    return lax.dot_general(a, b, (((1,), (1,)), ((), ())), preferred_element_type=F32)


def kernel(
    axes,
    text, image, prow, pcol,
    gt, gi, loss,
    t_own, tb, ib, pb, plan, gcol, s_own, sp, runm, runs, clcol, cl, rl, wb, gx, lbuf, lfin,
    loc, bsend, ri, rt, rp, rg, rs, rloss, rfin,
):
    z = lax.axis_index("grp_0")
    k = lax.axis_index("grp_1")
    other = 1 - k
    width = text.shape[1]
    ks = k * R

    sends = []

    def send(src, dst, rsem, **dev):
        copy = pltpu.make_async_remote_copy(
            src_ref=src,
            dst_ref=dst,
            send_sem=bsend.at[len(sends)],
            recv_sem=rsem,
            device_id=dev,
            device_id_type=MESH,
        )
        copy.start()
        sends.append(copy)

    def wait_for(dst, rsem):
        pltpu.make_async_remote_copy(
            src_ref=dst,
            dst_ref=dst,
            send_sem=bsend.at[0],
            recv_sem=rsem,
            device_id={"grp_1": other},
            device_id_type=MESH,
        ).wait_recv()

    def at_rows(ref, start):
        return ref.at[pl.ds(pl.multiple_of(start, R), R), :]

    def sem_of(sems, zz, n, kk):
        return sems.at[zz * (NC * KS) + n * KS + kk]

    def own_rows(ref, n):
        return ref.at[pl.ds(n * R, R), :]

    def load_own(base, with_text):
        copies = []

        def load(src, dst):
            copy = pltpu.make_async_copy(src, dst, loc.at[len(copies)])
            copy.start()
            copies.append(copy)

        for n in range(NC):
            load(own_rows(image, n), at_rows(ib, base(n) + ks))
        load(text, t_own)
        pb[z * KS + k] = prow[...]
        if with_text:
            for n in range(NC):
                load(own_rows(text, n), at_rows(tb, base(n) + ks))
        return copies

    def score_own(start, size):
        block = ib[pl.ds(start, size), :]
        s_own[:, pl.ds(start, size)] = dot_nt(t_own[...], block) * SCALE

    def text_gradient():
        tiles = [slice(t * LANES, (t + 1) * LANES) for t in range(NT)]
        for n in range(NC):
            rows = slice(n * R, (n + 1) * R)
            top = jnp.max(tree([s_own[rows, t] for t in tiles], jnp.maximum), axis=1, keepdims=True)
            total = jnp.sum(tree([jnp.exp(s_own[rows, t] - top) for t in tiles], add), axis=1, keepdims=True)
            row_lse = top + jnp.log(total)
            for t in tiles:
                s = s_own[rows, t]
                q = lax.broadcasted_iota(jnp.int32, (1, LANES), 1) + t.start
                hit = pcol[rows, :] == row_ids(q)
                w = jnp.exp(s - row_lse) + jnp.exp(s - cl[0:1, t]) - jnp.where(hit, 2.0, 0.0)
                wb[rows, t] = w.astype(BF16)
        for h in range(width // 256):
            cols = slice(h * 256, (h + 1) * 256)
            gt[:, cols] = jnp.dot(wb[...], ib[:, cols], preferred_element_type=F32) * (SCALE * 0.5)

    def finish():
        for copy in sends:
            copy.wait_send()
        sends.clear()

    barrier = pltpu.get_barrier_semaphore()

    def ends():
        far = 2 - z
        base = functools.partial(end_base, z)
        copies = load_own(base, False)
        pl.semaphore_signal(barrier, inc=1, device_id={"grp_1": other}, device_id_type=MESH)
        pl.semaphore_signal(barrier, inc=1, device_id={"grp_0": 1}, device_id_type=MESH)
        for copy in copies:
            copy.wait()
        pl.semaphore_wait(barrier, 2)

        def mine(n):
            return at_rows(ib, base(n) + ks)

        send(pb.at[z * KS + k], pb.at[z * KS + k], rp.at[z * KS + k], grp_0=1)
        for n in range(NC):
            send(mine(n), mine(n), sem_of(ri, z, n, k), grp_0=1)
        for n in range(NC):
            send(mine(n), mine(n), sem_of(ri, z, n, k), grp_1=other)
        for n in range(NC):
            send(own_rows(t_own, n), at_rows(tb, base(n) + ks), sem_of(rt, z, n, k), grp_0=1)

        for n in range(NC):
            part = at_rows(ib, mid_base(n) + ks)
            wait_for(part, sem_of(ri, 1, n, k))
            send(part, part, sem_of(ri, 1, n, k), grp_1=other)
        for n in range(NC):
            wait_for(at_rows(ib, base(n) + other * R), sem_of(ri, z, n, other))
            wait_for(at_rows(ib, mid_base(n) + other * R), sem_of(ri, 1, n, other))
        score_own(0, MIDW)
        for n in range(NC):
            part = at_rows(ib, end_base(far, n) + ks)
            wait_for(part, sem_of(ri, far, n, k))
            send(part, part, sem_of(ri, far, n, k), grp_1=other)
            wait_for(at_rows(ib, end_base(far, n) + other * R), sem_of(ri, far, n, other))
            score_own(MIDW + n * 2 * BLOCK, 2 * BLOCK)
        wait_for(cl, rs.at[0])
        text_gradient()
        for n in range(NC):
            part = gx.at[n, pl.ds(0, R), :]
            wait_for(part, rg.at[n])
            gi[n * R : (n + 1) * R, :] = gx[n, 0:R, :].astype(F32)
        wait_for(lfin, rfin.at[0])
        loss[...] = lfin[...]
        finish()

    def middle():
        copies = load_own(mid_base, True)
        pl.semaphore_signal(barrier, inc=1, device_id={"grp_1": other}, device_id_type=MESH)
        pl.semaphore_signal(barrier, inc=1, device_id={"grp_0": 0}, device_id_type=MESH)
        pl.semaphore_signal(barrier, inc=1, device_id={"grp_0": 2}, device_id_type=MESH)
        greeted = 3
        for name, size in axes:
            for step in range(1, size):
                peer = lax.rem(lax.axis_index(name) + step, size)
                pl.semaphore_signal(barrier, inc=1, device_id={name: peer}, device_id_type=MESH)
                greeted += 1
        for copy in copies:
            copy.wait()
        pl.semaphore_wait(barrier, greeted)

        def mine(ref, n):
            return at_rows(ref, mid_base(n) + ks)

        for n in range(NC):
            for e in (0, 2):
                send(mine(ib, n), mine(ib, n), sem_of(ri, 1, n, k), grp_0=e)
        send(pb.at[KS + k], pb.at[KS + k], rp.at[KS + k], grp_1=other)
        for n in range(NC):
            send(mine(ib, n), mine(ib, n), sem_of(ri, 1, n, k), grp_1=other)
        for n in range(NC):
            send(mine(tb, n), mine(tb, n), sem_of(rt, 1, n, k), grp_1=other)

        def ids(i, _):
            rows = pl.ds(pl.multiple_of(i * LANES, LANES), LANES)
            q = lax.broadcasted_iota(jnp.int32, (LANES, LANES), 0) + i * LANES
            gcol[rows, :] = row_ids(q)
            runm[rows, :] = jnp.full((LANES, LANES), -1e30, F32)
            runs[rows, :] = jnp.zeros((LANES, LANES), F32)
            return 0

        lax.fori_loop(0, NT, ids, 0)

        for e in (0, 2):
            slot = e * KS + k
            wait_for(pb.at[slot], rp.at[slot])
            send(pb.at[slot], pb.at[slot], rp.at[slot], grp_1=other)
        for n in range(NC):
            for e in (0, 2):
                part = at_rows(ib, end_base(e, n) + ks)
                wait_for(part, sem_of(ri, e, n, k))
                send(part, part, sem_of(ri, e, n, k), grp_0=2 - e)
                send(part, part, sem_of(ri, e, n, k), grp_1=other)
        for zz in range(ZS):
            wait_for(pb.at[zz * KS + other], rp.at[zz * KS + other])
            for n in range(NC):
                start = mid_base(n) if zz == 1 else end_base(zz, n)
                plan[0:1, start : start + BLOCK] = pb[zz * KS, n : n + 1, :] + pb[zz * KS + 1, n : n + 1, :]
        for n in range(NC):
            wait_for(at_rows(tb, mid_base(n) + other * R), sem_of(rt, 1, n, other))
            wait_for(at_rows(ib, mid_base(n) + other * R), sem_of(ri, 1, n, other))
            for e in (0, 2):
                wait_for(at_rows(ib, end_base(e, n) + other * R), sem_of(ri, e, n, other))
        score_own(0, TOTAL)

        def scores_and_stats(start, size, hits):
            sp[:, start : start + size] = dot_nt(ib[...], tb[start : start + size, :]) * SCALE
            tiles = [slice(start + t * LANES, start + (t + 1) * LANES) for t in range(size // LANES)]

            def first(i, carry):
                tops, hits = carry
                rows = pl.ds(pl.multiple_of(i * LANES, LANES), LANES)
                vs = [sp[rows, t] for t in tiles]
                old = runm[rows, :]
                top = jnp.maximum(jnp.max(tree(vs, jnp.maximum), axis=1, keepdims=True), old)
                fresh = jnp.sum(tree([jnp.exp(v - top) for v in vs], add), axis=1, keepdims=True)
                runs[rows, :] = runs[rows, :] * jnp.exp(old - top) + fresh
                runm[rows, :] = top
                ids = gcol[rows, :]
                found = [jnp.where(ids == plan[0:1, t], v, 0.0) for t, v in zip(tiles, vs)]
                hits = hits + fold(tree(found, add), add)
                return tuple(jnp.maximum(m, fold(v, jnp.maximum)) for m, v in zip(tops, vs)), hits

            none = jnp.full((8, LANES), -1e30, F32)
            tops, hits = lax.fori_loop(0, NT, first, (tuple(none for _ in tiles), hits))
            tops = [jnp.max(m, axis=0, keepdims=True) for m in tops]

            def second(i, sums):
                rows = pl.ds(pl.multiple_of(i * LANES, LANES), LANES)
                return tuple(s + fold(jnp.exp(sp[rows, t] - m), add) for s, t, m in zip(sums, tiles, tops))

            sums = lax.fori_loop(0, NT, second, tuple(jnp.zeros((8, LANES), F32) for _ in tiles))
            for t, m, s in zip(tiles, tops, sums):
                rl[0:1, t] = m + jnp.log(jnp.sum(s, axis=0, keepdims=True))
            return hits

        hits = scores_and_stats(0, MIDW, jnp.zeros((8, LANES), F32))
        for n in range(NC):
            for e in (0, 2):
                part = at_rows(tb, end_base(e, n) + ks)
                wait_for(part, sem_of(rt, e, n, k))
                send(part, part, sem_of(rt, e, n, k), grp_1=other)
            for e in (0, 2):
                wait_for(at_rows(tb, end_base(e, n) + other * R), sem_of(rt, e, n, other))
            hits = scores_and_stats(MIDW + n * 2 * BLOCK, 2 * BLOCK, hits)

        eye = lax.broadcasted_iota(jnp.int32, (LANES, LANES), 0) == lax.broadcasted_iota(jnp.int32, (LANES, LANES), 1)
        lse_sum = jnp.zeros((1, LANES), F32)
        for i in range(NT):
            rows = slice(i * LANES, (i + 1) * LANES)
            lse = runm[rows, :] + jnp.log(runs[rows, :])
            clcol[rows, :] = lse
            line = jnp.sum(fold(jnp.where(eye, lse, 0.0), add), axis=0, keepdims=True)
            cl[0:1, rows] = line
            lse_sum = lse_sum + line + rl[0:1, rows]
        part = jnp.sum(lse_sum, axis=1, keepdims=True) - 2.0 * jnp.sum(
            jnp.sum(hits, axis=0, keepdims=True), axis=1, keepdims=True
        )

        def weights(start, row):
            rows = pl.ds(pl.multiple_of(start, R), R)
            col = clcol[rows, :]
            ids = gcol[rows, :]
            for t in range(NT):
                lanes = slice(t * LANES, (t + 1) * LANES)
                s = sp[rows, lanes]
                hit = ids == plan[0:1, lanes]
                w = jnp.exp(s - col) + jnp.exp(s - rl[0:1, lanes]) - jnp.where(hit, 2.0, 0.0)
                wb[row : row + R, lanes] = w.astype(BF16)

        def exchange(name, size, off, value):
            me = lax.axis_index(name)
            lbuf[off + me] = jnp.broadcast_to(value, (8, LANES))
            for step in range(1, size):
                peer = lax.rem(me + step, size)
                send(lbuf.at[off + me], lbuf.at[off + me], rloss.at[off + me], **{name: peer})

        def collected(name, size, off):
            me = lax.axis_index(name)
            for step in range(1, size):
                peer = lax.rem(me + step, size)
                wait_for(lbuf.at[off + peer], rloss.at[off + peer])
            total = lbuf[off]
            for i in range(1, size):
                total = total + lbuf[off + i]
            return total[0:1, :]

        offs = [sum(size for _, size in axes[:i]) for i in range(len(axes))]
        exchange(*axes[0], offs[0], part)
        for e in (0, 2):
            send(cl, cl, rs.at[0], grp_0=e)

        for n in range(NC):
            weights(end_base(0, n) + ks, 0)
            weights(end_base(2, n) + ks, R)
            for h in range(width // 256):
                cols = slice(h * 256, (h + 1) * 256)
                g = jnp.dot(wb[0 : 2 * R, :], tb[:, cols], preferred_element_type=F32) * (SCALE * 0.5)
                gx[n, :, cols] = g.astype(BF16)
            for e in (0, 2):
                send(gx.at[n, pl.ds((e // 2) * R, R), :], gx.at[n, pl.ds(0, R), :], rg.at[n], grp_0=e)

        value = collected(*axes[0], offs[0])
        exchange(*axes[1], offs[1], value)
        for n in range(NC):
            weights(mid_base(n) + ks, n * R)
        for h in range(width // 256):
            cols = slice(h * 256, (h + 1) * 256)
            gi[:, cols] = jnp.dot(wb[...], tb[:, cols], preferred_element_type=F32) * (SCALE * 0.5)
        value = collected(*axes[1], offs[1])
        exchange(*axes[2], offs[2], value)
        text_gradient()
        value = collected(*axes[2], offs[2])
        groups = 1
        for _, size in axes:
            groups *= size
        lfin[...] = jnp.broadcast_to(value * (1.0 / (2.0 * TOTAL * groups)), (8, LANES))
        for e in (0, 2):
            send(lfin, lfin, rfin.at[0], grp_0=e)
        loss[...] = lfin[...]
        finish()

    pl.when(z != 1)(ends)
    pl.when(z == 1)(middle)


def local(axes, text, image, pair_index):
    rows, width = text.shape[1:]
    assert rows == ROWS
    pairs = pair_index[0]
    k = lax.axis_index("grp_1")
    pieces = pairs.reshape(NC, R)
    none = jnp.zeros_like(pieces)
    line = jnp.where(
        k == 0, jnp.concatenate([pieces, none], 1), jnp.concatenate([none, pieces], 1)
    )
    line = jnp.pad(line, ((0, 8 - NC), (0, 0)))
    column = jnp.broadcast_to(pairs[:, None], (rows, LANES))
    slots = sum(size for _, size in axes)
    vmem = pl.BlockSpec(memory_space=pltpu.VMEM)
    hbm = pl.BlockSpec(memory_space=pltpu.HBM)
    dma = pltpu.SemaphoreType.DMA
    gt, gi, loss = pl.pallas_call(
        functools.partial(kernel, axes),
        out_shape=(
            jax.ShapeDtypeStruct((rows, width), F32),
            jax.ShapeDtypeStruct((rows, width), F32),
            jax.ShapeDtypeStruct((8, LANES), F32),
        ),
        in_specs=[hbm, hbm, vmem, vmem],
        out_specs=[vmem, vmem, vmem],
        scratch_shapes=[
            pltpu.VMEM((rows, width), BF16),
            pltpu.VMEM((TOTAL, width), BF16),
            pltpu.VMEM((TOTAL, width), BF16),
            pltpu.VMEM((ZS * KS, 8, LANES), jnp.int32),
            pltpu.VMEM((1, TOTAL), jnp.int32),
            pltpu.VMEM((TOTAL, LANES), jnp.int32),
            pltpu.VMEM((rows, TOTAL), F32),
            pltpu.VMEM((TOTAL, TOTAL), F32),
            pltpu.VMEM((TOTAL, LANES), F32),
            pltpu.VMEM((TOTAL, LANES), F32),
            pltpu.VMEM((TOTAL, LANES), F32),
            pltpu.VMEM((1, TOTAL), F32),
            pltpu.VMEM((1, TOTAL), F32),
            pltpu.VMEM((rows, TOTAL), BF16),
            pltpu.VMEM((NC, 2 * R, width), BF16),
            pltpu.VMEM((slots, 8, LANES), F32),
            pltpu.VMEM((8, LANES), F32),
            dma((2 * NC + 2,)),
            dma((72,)),
            dma((ZS * NC * KS,)),
            dma((ZS * NC * KS,)),
            dma((ZS * KS,)),
            dma((NC,)),
            dma((1,)),
            dma((slots,)),
            dma((1,)),
        ],
        compiler_params=pltpu.CompilerParams(
            collective_id=0, has_side_effects=True, vmem_limit_bytes=48 * 1024 * 1024
        ),
    )(
        pltpu.with_memory_space_constraint(text[0], pltpu.HBM),
        pltpu.with_memory_space_constraint(image[0], pltpu.HBM),
        line,
        column,
    )
    return gt[None], gi[None], loss[0, 0]


def solution(mesh):
    torus = Mesh(mesh.devices.reshape(8, 4, 4, 3, 2), (*BLK, *GRP))
    axes = tuple((name, torus.shape[name]) for name in REDUCE)
    in_specs = (P(BLK, GRP, None), P(BLK, GRP, None), P(BLK, GRP))
    out_specs = (P(BLK, GRP, None), P(BLK, GRP, None), P())
    return jax.shard_map(
        functools.partial(local, axes), mesh=torus, in_specs=in_specs, out_specs=out_specs, check_vma=False
    )
```
